32 devices in a mesh: dp: 4 (over y, x), tensor: 8 (over z, core).
Axes of the slice: x: 2, y: 2, z: 4, core: 2. Of those that a mesh axis runs over, the one named last changes fastest.
Arguments:
- attention_output: bfloat16 [512, 8192], P('dp', 'tensor'), may hold values from -6 to 6
- residual: bfloat16 [512, 8192], P('dp', 'tensor'), may hold values from -6 to 6
- output_weight: bfloat16 [8192, 8192], P('tensor'), may hold values from -0.09375 to 0.09375
- down_factors: bfloat16 [256, 8192, 16], P('dp', 'tensor'), may hold values from -0.0625 to 0.0625
- up_factors: bfloat16 [256, 16, 8192], P('dp', None, 'tensor'), may hold values from -1.5 to 1.5
- adapter_index: int32 [512], P('dp'), may hold values from 0 to 255, as said below
Outputs:
- layer_out: bfloat16 [512, 8192], P('dp', 'tensor')
The draws below stay inside these ranges and needn't reach their ends.
Inputs may be any that keep to these rules, and one draw needn't show every extreme that they name: adapter_index // 64 is the request group that owns the adapter. Of one group's 128 rows at most 64 use adapters owned by one group, and in every draw some group owns the adapters of exactly 64 rows of every group.
All inputs are finite; a program needn't handle non-finite values.
Results may differ from the reference program's by a relative error of at most 0.0041.
Values may be sent and summed in bfloat16 or wider, within the bound.
A program may use at most 64 MiB of HBM per device.

```python
import jax
import jax.numpy as jnp
from jax import lax

MODEL_WIDTH = 8192
ADAPTER_RANK = 16
ADP_DEV = 64
ROWS = 128
ATTENTION_WIDTH = 8192
ADAPTER_COUNT = 256
CAP = 64
ROWS_ALL = 512
N_DP = 4


def draw_adapter_index(key, part):
    hot_key = jax.random.fold_in(key, 11)
    group_key = jax.random.fold_in(key, 23)
    hot_group = jax.random.randint(hot_key, (), 0, N_DP)

    def one_group(group_index):
        base_key = jax.random.fold_in(group_key, group_index)
        key_one = jax.random.fold_in(base_key, 1)
        key_two = jax.random.fold_in(base_key, 2)
        key_three = jax.random.fold_in(base_key, 3)
        key_four = jax.random.fold_in(base_key, 4)
        others = (hot_group + 1 + jnp.arange((N_DP - 1) * CAP) // CAP) % N_DP
        others = jax.random.permutation(key_one, others)[:ROWS - CAP]
        owners = jnp.concatenate([jnp.full((CAP,), hot_group, jnp.int32), others.astype(jnp.int32)])
        owners = jax.random.permutation(key_two, owners)
        top_bound = jax.random.randint(key_three, (ROWS,), 1, ADP_DEV + 1)
        local_index = jax.random.randint(key_four, (ROWS,), 0, ADP_DEV) % top_bound
        return owners * ADP_DEV + local_index
    table = jax.vmap(one_group)(jnp.arange(N_DP))
    return table.reshape(-1).astype(jnp.int32)


def strengthened(result, rng, source, target, parts, factor):
    def block_of(dim):
        return (jnp.arange(result.shape[dim]) // (result.shape[dim] // parts)).reshape((-1,) + (1,) * (result.ndim - 1 - dim))

    near = jax.random.permutation(rng, parts)[block_of(target)]
    far = (block_of(target) + parts // 2) % parts
    return jnp.where((block_of(source) == near) | (block_of(source) == far), factor * result, result)


def levels(stream_key, dims, cuts, least, high):
    loudness, own = 1.0, jax.random.fold_in(stream_key, 6)
    for axis_at, parts in cuts:
        steps = jnp.exp(jax.random.uniform(jax.random.fold_in(own, axis_at), (parts,), jnp.float32, least / len(cuts), high / len(cuts)))
        loudness = loudness * jnp.repeat(steps, dims[axis_at] // parts).reshape([-1 if axis == axis_at else 1 for axis in range(len(dims))])
    return loudness


def bell_draw(key, shape, scale, limit, cuts=(), kind=jnp.bfloat16):
    level = levels(key, shape, cuts, -0.22, 0.18) if cuts else 1.0
    result = jax.random.normal(key, shape, jnp.float32) * scale * level
    return jnp.minimum(jnp.maximum(result, -limit), limit).astype(kind)


def noise_with(stream_key, dims, deviation, reach, pieces, heavy, dtype=jnp.bfloat16):
    values = deviation * jax.random.normal(stream_key, dims, jnp.float32)
    if pieces:
        values = values * levels(stream_key, dims, pieces, -0.22, 0.18)
    return jnp.clip(strengthened(values, jax.random.fold_in(stream_key, 3), *heavy), -reach, reach).astype(dtype)


def setup_inputs(seed: int = 0) -> dict:
    keys = jax.random.split(jax.random.key(seed), 7)
    attention_output = bell_draw(keys[0], (ROWS_ALL, ATTENTION_WIDTH), 1.0, 6.0, ((0, 4), (1, 8)))
    residual = bell_draw(keys[1], (ROWS_ALL, MODEL_WIDTH), 1.0, 6.0, ((0, 4), (1, 8)))
    output_weight = noise_with(keys[2], (ATTENTION_WIDTH, MODEL_WIDTH), ATTENTION_WIDTH ** -0.5, 0.09375, ((0, 8),), (0, 1, 8, 2.0))
    down_factors = bell_draw(keys[3], (ADAPTER_COUNT, ATTENTION_WIDTH, ADAPTER_RANK), ATTENTION_WIDTH ** -0.5, 0.0625, ((0, 4), (1, 8)))
    up_factors = bell_draw(keys[4], (ADAPTER_COUNT, ADAPTER_RANK, MODEL_WIDTH), ADAPTER_RANK ** -0.5, 1.5, ((0, 4), (2, 8)))
    adapter_index = draw_adapter_index(jax.random.fold_in(keys[6], 71), 0)
    return {"attention_output": attention_output, "residual": residual, "output_weight": output_weight, "down_factors": down_factors, "up_factors": up_factors, "adapter_index": adapter_index}


def reference(attention_output, residual, output_weight, down_factors, up_factors, adapter_index):
    base_out = jnp.dot(attention_output, output_weight, preferred_element_type=jnp.float32)
    blocks = ROWS_ALL // ROWS

    def branch(block_in):
        x_rows, row_indices = block_in
        selected_down = down_factors[row_indices].astype(jnp.float32)
        shrink = jnp.einsum("rk,rkj->rj", x_rows.astype(jnp.float32), selected_down).astype(jnp.bfloat16)
        selected_up = up_factors[row_indices].astype(jnp.float32)
        return jnp.einsum("rj,rjc->rc", shrink.astype(jnp.float32), selected_up).astype(jnp.bfloat16)

    expand = lax.map(branch, (attention_output.reshape(blocks, ROWS, ATTENTION_WIDTH), adapter_index.reshape(blocks, ROWS)))
    expand = expand.reshape(ROWS_ALL, MODEL_WIDTH)
    total = residual.astype(jnp.float32) + base_out + expand.astype(jnp.float32)
    return total.astype(jnp.bfloat16)
```

```python
import functools

import jax
import jax.numpy as jnp
from jax import lax
from jax.experimental import pallas as pl
from jax.experimental.pallas import tpu as pltpu
from jax.sharding import PartitionSpec as P

MESH = pl.DeviceIdType.MESH
F32 = jnp.float32
BF16 = jnp.bfloat16
LANES = 128
PIECES = 2


def kernel(
    groups, members, rank, owned,
    x_ref, res_ref, idx_ref, w_ref, down_ref, up_ref, out_ref,
    wbuf, dbuf, ubuf, own, psend, precv, rrecv, lrecv, rsend, lsend,
    xsend, xrecv, terms, packed, arp, arz, esend, eback,
    w_sem, d_sem, ps_sem, pr_sem, rs_sem, rr_sem, ls_sem, lr_sem,
    xs_sem, xr_sem, as_sem, ar_sem, zs_sem, zr_sem, es_sem, er_sem,
):
    chips = members // 2
    g = lax.axis_index("dp")
    t = lax.axis_index("tensor")
    z = t // 2
    c = lax.rem(t, 2)
    partner = z * 2 + (1 - c)
    rows, depth = x_ref.shape
    width = out_ref.shape[1]
    cap = xrecv.shape[1]
    slots = groups * cap
    low = z < chips // 2

    def block_chip(i):
        return jnp.where(low, chips - 1 - i, i)

    def weight_copy(i, which):
        column = block_chip(i) * 2 + jnp.where(which == 0, 1 - c, c)
        start = pl.multiple_of(column * width, LANES)
        return pltpu.make_async_copy(
            w_ref.at[:, pl.ds(start, width)], wbuf.at[2 * i + which], w_sem.at[2 * i + which]
        )

    down_copy = pltpu.make_async_copy(down_ref, dbuf, d_sem.at[0])
    up_copy = pltpu.make_async_copy(up_ref, ubuf, d_sem.at[1])
    for i in range(chips):
        for which in range(2):
            weight_copy(i, which).start()
        if i == 0:
            down_copy.start()
    up_copy.start()

    barrier = pltpu.get_barrier_semaphore()
    pl.semaphore_signal(barrier, inc=1, device_id=(g, partner), device_id_type=MESH)
    for k in range(1, chips):
        peer = lax.rem(z + k, chips) * 2 + c
        pl.semaphore_signal(barrier, inc=1, device_id=(g, peer), device_id_type=MESH)
    for k in range(1, groups):
        pl.semaphore_signal(
            barrier, inc=1, device_id=(lax.rem(g + k, groups), t), device_id_type=MESH
        )

    idx_row = idx_ref[...]
    r_i = lax.broadcasted_iota(jnp.int32, (rows, rows), 0)
    c_i = lax.broadcasted_iota(jnp.int32, (rows, rows), 1)
    idx_full = jnp.broadcast_to(idx_row, (rows, rows))
    idx_col = jnp.sum(jnp.where(r_i == c_i, idx_full, 0), axis=1, keepdims=True)
    own_row = idx_row // owned
    own_col = idx_col // owned
    same = own_col == own_row
    rank_row = jnp.sum(jnp.where(same & (r_i < c_i), 1, 0), axis=0, keepdims=True)
    rank_col = jnp.sum(jnp.where(same & (c_i < r_i), 1, 0), axis=1, keepdims=True)
    slot_row = rank_row + own_row * cap
    slot_col = rank_col + own_col * cap
    number_row = lax.rem(idx_row, owned) + 1
    placing = lax.broadcasted_iota(jnp.int32, (slots, rows), 0) == slot_row
    request = jnp.sum(jnp.where(placing, number_row, 0), axis=1, keepdims=True)
    place = jnp.where(placing, 1.0, 0.0).astype(BF16)
    for k in range(groups):
        xsend[k, :, depth:] = jnp.broadcast_to(
            request[k * cap:(k + 1) * cap].astype(F32), (cap, LANES)
        ).astype(BF16)
    step = min(256, depth)
    for j in range(depth // step):
        moved = jnp.dot(
            place, x_ref[:, j * step:(j + 1) * step], preferred_element_type=F32
        ).astype(BF16)
        for k in range(groups):
            xsend[k, :, j * step:(j + 1) * step] = moved[k * cap:(k + 1) * cap]

    pl.semaphore_wait(barrier, chips + groups - 1)

    def row_copy(k):
        to = lax.rem(g + k, groups)
        return pltpu.make_async_remote_copy(
            src_ref=xsend.at[to], dst_ref=xrecv.at[g], send_sem=xs_sem.at[k - 1],
            recv_sem=xr_sem.at[g], device_id=(to, t), device_id_type=MESH,
        )

    def row_wait(k):
        source = lax.rem(g + k, groups)
        pltpu.make_async_remote_copy(
            src_ref=xsend.at[source], dst_ref=xrecv.at[source], send_sem=xs_sem.at[k - 1],
            recv_sem=xr_sem.at[source], device_id=(source, t), device_id_type=MESH,
        ).wait_recv()

    for k in range(1, groups):
        row_copy(k).start()
    xrecv[g] = xsend[g]

    tile = min(256, width)
    tiles = width // tile

    def pair_copy(chip):
        return pltpu.make_async_remote_copy(
            src_ref=psend.at[chip], dst_ref=precv.at[chip], send_sem=ps_sem.at[chip],
            recv_sem=pr_sem.at[chip], device_id=(g, partner), device_id_type=MESH,
        )

    def project(i):
        chip = block_chip(i)
        weight_copy(i, 0).wait()

        @pl.loop(0, tiles)
        def _(n):
            cols = pl.ds(pl.multiple_of(n * tile, LANES), tile)
            psend[chip, :, cols] = jnp.dot(
                x_ref[...], wbuf[2 * i, :, cols], preferred_element_type=F32
            ).astype(BF16)

        pair_copy(chip).start()
        weight_copy(i, 1).wait()

        @pl.loop(0, tiles)
        def _(n):
            cols = pl.ds(pl.multiple_of(n * tile, LANES), tile)
            own[chip, :, cols] = jnp.dot(
                x_ref[...], wbuf[2 * i + 1, :, cols], preferred_element_type=F32
            )

    piece = rows // PIECES
    strip = 16

    def hop(chip, q, to, send, recv, s_sem, r_sem):
        k = chip * PIECES + q
        part = pl.ds(q * piece, piece)
        return pltpu.make_async_remote_copy(
            src_ref=send.at[chip, part], dst_ref=recv.at[chip, part], send_sem=s_sem.at[k],
            recv_sem=r_sem.at[k], device_id=(g, to * 2 + c), device_id_type=MESH,
        )

    right = functools.partial(hop, send=rsend, recv=rrecv, s_sem=rs_sem, r_sem=rr_sem)
    left = functools.partial(hop, send=lsend, recv=lrecv, s_sem=ls_sem, r_sem=lr_sem)

    def pass_on(chip, q, first, to, make, send, recv):
        @pl.when(first)
        def _():
            @pl.loop(0, piece // strip)
            def _(n):
                at = pl.ds(pl.multiple_of(q * piece + n * strip, strip), strip)
                send[chip, at] = (own[chip, at] + precv[chip, at].astype(F32)).astype(BF16)

        @pl.when(jnp.logical_not(first))
        def _():
            make(chip, q, to).wait_recv()

            @pl.loop(0, piece // strip)
            def _(n):
                at = pl.ds(pl.multiple_of(q * piece + n * strip, strip), strip)
                send[chip, at] = (
                    own[chip, at] + precv[chip, at].astype(F32) + recv[chip, at].astype(F32)
                ).astype(BF16)

        make(chip, q, to).start()

    def chain(turn, q):
        @pl.when(z <= turn)
        def _():
            pass_on(chips - 1 - turn + z, q, z == 0, z + 1, right, rsend, rrecv)

        @pl.when(chips - 1 - z <= turn)
        def _():
            pass_on(turn - chips + 1 + z, q, z == chips - 1, z - 1, left, lsend, lrecv)

    project(0)
    if chips > 1:
        project(1)
    pair_copy(block_chip(0)).wait_recv()
    for q in range(PIECES):
        chain(0, q)
    for i in range(2, chips):
        project(i)
    for i in range(1, chips):
        pair_copy(block_chip(i)).wait_recv()
    if chips > 2:
        chain(1, 0)

    for k in range(1, groups):
        row_wait(k)
    down_copy.wait()
    lane_group = lax.broadcasted_iota(jnp.int32, (slots, LANES), 1) // rank
    lane_number = (lane_group + 1).astype(F32)
    per_tile = LANES // rank
    tile_count = owned * rank // LANES
    wanted = xrecv[:, :, depth:].reshape(slots, LANES).astype(F32)
    flat = xrecv[:, :, :depth].reshape(slots, depth)
    terms[...] = jnp.zeros_like(terms)
    pair = 2 if tile_count % 2 == 0 else 1

    @pl.loop(0, tile_count // pair)
    def _(m):
        at = pl.ds(pl.multiple_of(m * pair * LANES, LANES), pair * LANES)
        every = lax.dot_general(
            flat, dbuf[at, :], (((1,), (1,)), ((), ())), preferred_element_type=F32
        )
        for p in range(pair):
            first_number = ((m * pair + p) * per_tile).astype(F32)
            terms[...] += jnp.where(
                wanted == lane_number + first_number, every[:, p * LANES:(p + 1) * LANES], 0.0
            )

    def spread_lanes(v):
        shift = rank
        while shift < LANES:
            v = v + pltpu.roll(v, shift, 1)
            shift *= 2
        return v

    pack_rows = slots // per_tile
    pack_group = lax.broadcasted_iota(jnp.int32, (pack_rows, LANES), 1) // rank
    chosen_terms = spread_lanes(terms[...])
    mine = jnp.zeros((pack_rows, LANES), F32)
    for p in range(per_tile):
        mine = jnp.where(
            pack_group == p, chosen_terms[p * pack_rows:(p + 1) * pack_rows], mine
        )
    packed[...] = mine
    term_pair = pltpu.make_async_remote_copy(
        src_ref=packed, dst_ref=arp, send_sem=as_sem.at[0], recv_sem=ar_sem.at[0],
        device_id=(g, partner), device_id_type=MESH,
    )
    term_pair.start()
    if chips > 2:
        for q in range(1, PIECES):
            chain(1, q)
    term_pair.wait_recv()
    arz[z] = packed[...] + arp[...]

    def term_copy(k):
        to = lax.rem(z + k, chips)
        return pltpu.make_async_remote_copy(
            src_ref=arz.at[z], dst_ref=arz.at[z], send_sem=zs_sem.at[k - 1],
            recv_sem=zr_sem.at[z], device_id=(g, to * 2 + c), device_id_type=MESH,
        )

    def term_wait(k):
        source = lax.rem(z + k, chips)
        pltpu.make_async_remote_copy(
            src_ref=arz.at[source], dst_ref=arz.at[source], send_sem=zs_sem.at[k - 1],
            recv_sem=zr_sem.at[source], device_id=(g, source * 2 + c), device_id_type=MESH,
        ).wait_recv()

    for k in range(1, chips):
        term_copy(k).start()
    for k in range(1, chips):
        term_wait(k)
    total = arz[0]
    for k in range(1, chips):
        total = total + arz[k]
    total = total.astype(BF16).astype(F32)

    up_copy.wait()
    shrink = jnp.concatenate(
        [spread_lanes(jnp.where(pack_group == p, total, 0.0)) for p in range(per_tile)], axis=0
    )
    spread = jnp.concatenate(
        [
            jnp.where(wanted == lane_number + float(m * per_tile), shrink, 0.0).astype(BF16)
            for m in range(tile_count)
        ],
        axis=1,
    )

    @pl.loop(0, tiles)
    def _(n):
        cols = pl.ds(pl.multiple_of(n * tile, LANES), tile)
        grown = jnp.dot(spread, ubuf[:, cols], preferred_element_type=F32).astype(BF16)
        for k in range(groups):
            esend[k, :, cols] = grown[k * cap:(k + 1) * cap]

    def back_copy(k):
        to = lax.rem(g + k, groups)
        return pltpu.make_async_remote_copy(
            src_ref=esend.at[to], dst_ref=eback.at[g], send_sem=es_sem.at[k - 1],
            recv_sem=er_sem.at[g], device_id=(to, t), device_id_type=MESH,
        )

    def back_wait(k):
        source = lax.rem(g + k, groups)
        pltpu.make_async_remote_copy(
            src_ref=esend.at[source], dst_ref=eback.at[source], send_sem=es_sem.at[k - 1],
            recv_sem=er_sem.at[source], device_id=(source, t), device_id_type=MESH,
        ).wait_recv()

    for k in range(1, groups):
        back_copy(k).start()
    eback[g] = esend[g]

    for turn in range(2, chips - 1):
        for q in range(PIECES):
            chain(turn, q)

    for k in range(1, groups):
        back_wait(k)
    unplace = jnp.where(
        lax.broadcasted_iota(jnp.int32, (rows, slots), 1) == slot_col, 1.0, 0.0
    ).astype(BF16)

    @pl.loop(0, tiles)
    def _(n):
        cols = pl.ds(pl.multiple_of(n * tile, LANES), tile)
        back = eback[:, :, cols].reshape(slots, tile)
        branch = jnp.dot(unplace, back, preferred_element_type=F32)
        own[z, :, cols] = (
            own[z, :, cols] + precv[z, :, cols].astype(F32)
            + res_ref[:, cols].astype(F32) + branch
        )

    for q in range(PIECES):
        part = slice(q * piece, (q + 1) * piece)

        @pl.when(z > 0)
        def _():
            right(z, q, z).wait_recv()

            @pl.loop(0, piece // strip)
            def _(n):
                at = pl.ds(pl.multiple_of(q * piece + n * strip, strip), strip)
                own[z, at] = own[z, at] + rrecv[z, at].astype(F32)

        @pl.when(z < chips - 1)
        def _():
            left(z, q, z).wait_recv()

            @pl.loop(0, piece // strip)
            def _(n):
                at = pl.ds(pl.multiple_of(q * piece + n * strip, strip), strip)
                own[z, at] = own[z, at] + lrecv[z, at].astype(F32)

        @pl.loop(0, piece // strip)
        def _(n):
            at = pl.ds(pl.multiple_of(q * piece + n * strip, strip), strip)
            out_ref[at] = own[z, at].astype(BF16)

    for i in range(chips):
        pair_copy(i).wait_send()
    for k in range(1, groups):
        row_copy(k).wait_send()
        back_copy(k).wait_send()
    term_pair.wait_send()
    for k in range(1, chips):
        term_copy(k).wait_send()
    for chip in range(chips):
        for q in range(PIECES):
            @pl.when(z < chip)
            def _():
                right(chip, q, z + 1).wait_send()

            @pl.when(z > chip)
            def _():
                left(chip, q, z - 1).wait_send()


def body(attention_output, residual, output_weight, down_factors, up_factors, adapter_index):
    groups = lax.axis_size("dp")
    members = lax.axis_size("tensor")
    rows, depth = attention_output.shape
    owned, _, rank = down_factors.shape
    width = output_weight.shape[1] // members
    cap = 2 * rows // groups
    chips = members // 2
    slots = groups * cap
    down = jnp.swapaxes(down_factors, 1, 2).reshape(owned * rank, depth)
    up = up_factors.reshape(owned * rank, width)
    vmem = pl.BlockSpec(memory_space=pltpu.VMEM)
    hbm = pl.BlockSpec(memory_space=pl.ANY)
    dma = pltpu.SemaphoreType.DMA
    hops = chips * PIECES
    return pl.pallas_call(
        functools.partial(kernel, groups, members, rank, owned),
        out_shape=jax.ShapeDtypeStruct((rows, width), BF16),
        in_specs=[vmem, vmem, vmem, hbm, hbm, hbm],
        out_specs=vmem,
        scratch_shapes=[
            pltpu.VMEM((members, depth, width), BF16),
            pltpu.VMEM((owned * rank, depth), BF16),
            pltpu.VMEM((owned * rank, width), BF16),
            pltpu.VMEM((chips, rows, width), F32),
            pltpu.VMEM((chips, rows, width), BF16),
            pltpu.VMEM((chips, rows, width), BF16),
            pltpu.VMEM((chips, rows, width), BF16),
            pltpu.VMEM((chips, rows, width), BF16),
            pltpu.VMEM((chips, rows, width), BF16),
            pltpu.VMEM((chips, rows, width), BF16),
            pltpu.VMEM((groups, cap, depth + LANES), BF16),
            pltpu.VMEM((groups, cap, depth + LANES), BF16),
            pltpu.VMEM((slots, LANES), F32),
            pltpu.VMEM((slots * rank // LANES, LANES), F32),
            pltpu.VMEM((slots * rank // LANES, LANES), F32),
            pltpu.VMEM((chips, slots * rank // LANES, LANES), F32),
            pltpu.VMEM((groups, cap, width), BF16),
            pltpu.VMEM((groups, cap, width), BF16),
            dma((members,)), dma((2,)),
            dma((chips,)), dma((chips,)),
            dma((hops,)), dma((hops,)), dma((hops,)), dma((hops,)),
            dma((groups,)), dma((groups,)),
            dma((1,)), dma((1,)),
            dma((chips,)), dma((chips,)),
            dma((groups,)), dma((groups,)),
        ],
        compiler_params=pltpu.CompilerParams(
            collective_id=0, has_side_effects=True, vmem_limit_bytes=60 * 1024 * 1024
        ),
    )(attention_output, residual, adapter_index.reshape(1, rows), output_weight, down, up)


def solution(mesh):
    return jax.shard_map(
        body,
        mesh=mesh,
        in_specs=(
            P("dp", "tensor"),
            P("dp", "tensor"),
            P("tensor", None),
            P("dp", "tensor", None),
            P("dp", None, "tensor"),
            P("dp"),
        ),
        out_specs=P("dp", "tensor"),
        check_vma=False,
    )
```

```python
import functools

import jax
import jax.numpy as jnp
from jax import lax
from jax.experimental import pallas as pl
from jax.experimental.pallas import tpu as pltpu
from jax.sharding import PartitionSpec as P

MESH = pl.DeviceIdType.MESH
F32 = jnp.float32
BF16 = jnp.bfloat16
LANES = 128
PIECES = 2
AHEAD = 3


def kernel(
    groups, members, rank, owned, halves,
    x_ref, res_ref, idx_ref, w_ref, down_ref, up_ref, out_ref,
    wbuf, dbuf, ubuf, rbuf, own, psend, precv, rrecv, lrecv, rsend, lsend,
    xsend, xrecv, terms, packed, arp, arz, esend, eback,
    w_sem, d_sem, ps_sem, pr_sem, rs_sem, rr_sem, ls_sem, lr_sem,
    xs_sem, xr_sem, as_sem, ar_sem, zs_sem, zr_sem, es_sem, er_sem,
):
    chips = members // 2
    g = lax.axis_index("dp")
    t = lax.axis_index("tensor")
    z = t // 2
    c = lax.rem(t, 2)
    partner = z * 2 + (1 - c)
    rows, depth = x_ref.shape
    width = out_ref.shape[1]
    part = xrecv.shape[2]
    cap = part * halves
    slots = groups * part
    low = z < chips // 2
    piece = width // PIECES

    def block_chip(i):
        return jnp.where(low, chips - 1 - i, i)

    def weight_copy(n):
        column = block_chip(n // 2) * 2 + (1 - c if n % 2 == 0 else c)
        start = pl.multiple_of(column * width, LANES)
        return pltpu.make_async_copy(
            w_ref.at[:, pl.ds(start, width)], wbuf.at[n], w_sem.at[n]
        )

    down_copy = pltpu.make_async_copy(down_ref, dbuf, d_sem.at[0])
    up_copy = pltpu.make_async_copy(up_ref, ubuf, d_sem.at[1])
    res_copy = pltpu.make_async_copy(res_ref, rbuf, d_sem.at[2])
    for n in range(min(AHEAD, members)):
        weight_copy(n).start()

    barrier = pltpu.get_barrier_semaphore()
    pl.semaphore_signal(barrier, inc=1, device_id=(g, partner), device_id_type=MESH)
    for k in range(1, chips):
        peer = lax.rem(z + k, chips) * 2 + c
        pl.semaphore_signal(barrier, inc=1, device_id=(g, peer), device_id_type=MESH)
    for k in range(1, groups):
        pl.semaphore_signal(
            barrier, inc=1, device_id=(lax.rem(g + k, groups), t), device_id_type=MESH
        )

    idx_row = idx_ref[...]
    r_i = lax.broadcasted_iota(jnp.int32, (rows, rows), 0)
    c_i = lax.broadcasted_iota(jnp.int32, (rows, rows), 1)
    idx_full = jnp.broadcast_to(idx_row, (rows, rows))
    idx_col = jnp.sum(jnp.where(r_i == c_i, idx_full, 0), axis=1, keepdims=True)
    own_row = idx_row // owned
    own_col = idx_col // owned
    same = own_col == own_row
    rank_row = jnp.sum(jnp.where(same & (r_i < c_i), 1, 0), axis=0, keepdims=True)
    rank_col = jnp.sum(jnp.where(same & (c_i < r_i), 1, 0), axis=1, keepdims=True)

    def slot_of(place_rank, owner, h):
        inside = place_rank - h * part
        keep = (inside >= 0) & (inside < part)
        return jnp.where(keep, owner * part + inside, -1)

    number_row = lax.rem(idx_row, owned) + 1
    step = min(256, depth)

    def row_copy(h, k):
        to = lax.rem(g + k, groups)
        return pltpu.make_async_remote_copy(
            src_ref=xsend.at[h, to], dst_ref=xrecv.at[h, g],
            send_sem=xs_sem.at[h * groups + k], recv_sem=xr_sem.at[h * groups + g],
            device_id=(to, t), device_id_type=MESH,
        )

    def row_wait(h, k):
        source = lax.rem(g + k, groups)
        pltpu.make_async_remote_copy(
            src_ref=xsend.at[h, source], dst_ref=xrecv.at[h, source],
            send_sem=xs_sem.at[h * groups + k], recv_sem=xr_sem.at[h * groups + source],
            device_id=(source, t), device_id_type=MESH,
        ).wait_recv()

    for h in range(halves):
        slot_row = slot_of(rank_row, own_row, h)
        placing = lax.broadcasted_iota(jnp.int32, (slots, rows), 0) == slot_row
        request = jnp.sum(jnp.where(placing, number_row, 0), axis=1, keepdims=True)
        place = jnp.where(placing, 1.0, 0.0).astype(BF16)
        numbers = jnp.broadcast_to(request.astype(F32), (slots, LANES)).astype(BF16)
        for k in range(groups):
            xsend[h, k, :, depth:] = numbers[k * part:(k + 1) * part]
        for j in range(depth // step):
            moved = jnp.dot(
                place, x_ref[:, j * step:(j + 1) * step], preferred_element_type=F32
            ).astype(BF16)
            for k in range(groups):
                xsend[h, k, :, j * step:(j + 1) * step] = moved[k * part:(k + 1) * part]
        if h == 0:
            pl.semaphore_wait(barrier, chips + groups - 1)
        for k in range(1, groups):
            row_copy(h, k).start()
        xrecv[h, g] = xsend[h, g]
        if h == 0:
            down_copy.start()

    tile = min(256, piece)
    tiles = piece // tile

    def pair_copy(chip, q):
        k = chip * PIECES + q
        return pltpu.make_async_remote_copy(
            src_ref=psend.at[k], dst_ref=precv.at[k], send_sem=ps_sem.at[k],
            recv_sem=pr_sem.at[k], device_id=(g, partner), device_id_type=MESH,
        )

    strip = 16

    def hop(chip, q, to, send, recv, s_sem, r_sem):
        k = chip * PIECES + q
        return pltpu.make_async_remote_copy(
            src_ref=send.at[k], dst_ref=recv.at[k], send_sem=s_sem.at[k],
            recv_sem=r_sem.at[k], device_id=(g, to * 2 + c), device_id_type=MESH,
        )

    right = functools.partial(hop, send=rsend, recv=rrecv, s_sem=rs_sem, r_sem=rr_sem)
    left = functools.partial(hop, send=lsend, recv=lrecv, s_sem=ls_sem, r_sem=lr_sem)

    def pass_on(chip, q, first, to, make, send, recv):
        k = chip * PIECES + q

        @pl.when(first)
        def _():
            @pl.loop(0, rows // strip)
            def _(n):
                at = pl.ds(pl.multiple_of(n * strip, strip), strip)
                send[k, at] = (own[k, at] + precv[k, at].astype(F32)).astype(BF16)

        @pl.when(jnp.logical_not(first))
        def _():
            make(chip, q, to).wait_recv()

            @pl.loop(0, rows // strip)
            def _(n):
                at = pl.ds(pl.multiple_of(n * strip, strip), strip)
                send[k, at] = (
                    own[k, at] + precv[k, at].astype(F32) + recv[k, at].astype(F32)
                ).astype(BF16)

        make(chip, q, to).start()

    def chain(turn, q):
        @pl.when(z <= turn)
        def _():
            pass_on(chips - 1 - turn + z, q, z == 0, z + 1, right, rsend, rrecv)

        @pl.when(chips - 1 - z <= turn)
        def _():
            pass_on(turn - chips + 1 + z, q, z == chips - 1, z - 1, left, lsend, lrecv)

    def start_weights(n):
        if n + AHEAD < members:
            weight_copy(n + AHEAD).start()

    def project(i):
        chip = block_chip(i)
        weight_copy(2 * i).wait()
        start_weights(2 * i)
        for q in range(PIECES):
            for n in range(tiles):
                psend[chip * PIECES + q, :, n * tile:(n + 1) * tile] = jnp.dot(
                    x_ref[...],
                    wbuf[2 * i, :, q * piece + n * tile:q * piece + (n + 1) * tile],
                    preferred_element_type=F32,
                ).astype(BF16)
            pair_copy(chip, q).start()
        weight_copy(2 * i + 1).wait()
        start_weights(2 * i + 1)
        for q in range(PIECES):
            for n in range(tiles):
                own[chip * PIECES + q, :, n * tile:(n + 1) * tile] = jnp.dot(
                    x_ref[...],
                    wbuf[2 * i + 1, :, q * piece + n * tile:q * piece + (n + 1) * tile],
                    preferred_element_type=F32,
                )
            if i == 0:
                pair_copy(chip, q).wait_recv()
                if chips > 1:
                    chain(0, q)

    def paired(i):
        for q in range(PIECES):
            pair_copy(block_chip(i), q).wait_recv()

    lane_group = lax.broadcasted_iota(jnp.int32, (slots, LANES), 1) // rank
    lane_number = (lane_group + 1).astype(F32)
    per_tile = LANES // rank
    tile_count = owned * rank // LANES
    pair = 2 if tile_count % 2 == 0 else 1
    pack_rows = slots // per_tile
    pack_group = lax.broadcasted_iota(jnp.int32, (pack_rows, LANES), 1) // rank

    def spread_lanes(v):
        shift = rank
        while shift < LANES:
            v = v + pltpu.roll(v, shift, 1)
            shift *= 2
        return v

    def term_pair(h):
        return pltpu.make_async_remote_copy(
            src_ref=packed.at[h], dst_ref=arp.at[h], send_sem=as_sem.at[h],
            recv_sem=ar_sem.at[h], device_id=(g, partner), device_id_type=MESH,
        )

    def term_copy(h, k):
        to = lax.rem(z + k, chips)
        return pltpu.make_async_remote_copy(
            src_ref=arz.at[h, z], dst_ref=arz.at[h, z], send_sem=zs_sem.at[h * chips + k],
            recv_sem=zr_sem.at[h * chips + z], device_id=(g, to * 2 + c), device_id_type=MESH,
        )

    def term_wait(h, k):
        source = lax.rem(z + k, chips)
        pltpu.make_async_remote_copy(
            src_ref=arz.at[h, source], dst_ref=arz.at[h, source],
            send_sem=zs_sem.at[h * chips + k], recv_sem=zr_sem.at[h * chips + source],
            device_id=(g, source * 2 + c), device_id_type=MESH,
        ).wait_recv()

    def wanted_of(h):
        return xrecv[h, :, :, depth:].reshape(slots, LANES).astype(F32)

    def shrink_rows(h):
        for k in range(1, groups):
            row_wait(h, k)
        if h == 0:
            down_copy.wait()
            up_copy.start()
            res_copy.start()
        wanted = wanted_of(h)
        flat = xrecv[h, :, :, :depth].reshape(slots, depth)
        terms[...] = jnp.zeros_like(terms)

        @pl.loop(0, tile_count // pair)
        def _(m):
            at = pl.ds(pl.multiple_of(m * pair * LANES, LANES), pair * LANES)
            every = lax.dot_general(
                flat, dbuf[at, :], (((1,), (1,)), ((), ())), preferred_element_type=F32
            )
            for p in range(pair):
                first_number = ((m * pair + p) * per_tile).astype(F32)
                terms[...] += jnp.where(
                    wanted == lane_number + first_number, every[:, p * LANES:(p + 1) * LANES], 0.0
                )

        chosen_terms = spread_lanes(terms[...])
        mine = jnp.zeros((pack_rows, LANES), F32)
        for p in range(per_tile):
            mine = jnp.where(
                pack_group == p, chosen_terms[p * pack_rows:(p + 1) * pack_rows], mine
            )
        packed[h] = mine
        term_pair(h).start()

    def sum_send(h):
        term_pair(h).wait_recv()
        arz[h, z] = packed[h] + arp[h]
        for k in range(1, chips):
            term_copy(h, k).start()

    def back_copy(h, k):
        to = lax.rem(g + k, groups)
        return pltpu.make_async_remote_copy(
            src_ref=esend.at[h, to], dst_ref=eback.at[h, g],
            send_sem=es_sem.at[h * groups + k], recv_sem=er_sem.at[h * groups + g],
            device_id=(to, t), device_id_type=MESH,
        )

    def back_wait(h, k):
        source = lax.rem(g + k, groups)
        pltpu.make_async_remote_copy(
            src_ref=esend.at[h, source], dst_ref=eback.at[h, source],
            send_sem=es_sem.at[h * groups + k], recv_sem=er_sem.at[h * groups + source],
            device_id=(source, t), device_id_type=MESH,
        ).wait_recv()

    wide = min(256, width)

    def expand_rows(h):
        for k in range(1, chips):
            term_wait(h, k)
        total = arz[h, 0]
        for k in range(1, chips):
            total = total + arz[h, k]
        total = total.astype(BF16).astype(F32)
        if h == 0:
            up_copy.wait()
        wanted = wanted_of(h)
        shrink = jnp.concatenate(
            [spread_lanes(jnp.where(pack_group == p, total, 0.0)) for p in range(per_tile)],
            axis=0,
        )
        spread = jnp.concatenate(
            [
                jnp.where(wanted == lane_number + float(m * per_tile), shrink, 0.0).astype(BF16)
                for m in range(tile_count)
            ],
            axis=1,
        )

        @pl.loop(0, width // wide)
        def _(n):
            cols = pl.ds(pl.multiple_of(n * wide, LANES), wide)
            grown = jnp.dot(spread, ubuf[:, cols], preferred_element_type=F32).astype(BF16)
            for k in range(groups):
                esend[h, k, :, cols] = grown[k * part:(k + 1) * part]

        for k in range(1, groups):
            back_copy(h, k).start()
        eback[h, g] = esend[h, g]

    last = halves - 1
    early = chips // 2
    project(0)
    if chips > 1:
        project(1)
    shrink_rows(0)
    for i in range(2, chips):
        project(i)
        paired(i - 1)
        if i == 2:
            sum_send(0)
        if i - 1 < early and i - 1 < chips - 1:
            chain(i - 1, 0)
        if i == 2 and halves > 1:
            shrink_rows(1)
        if i - 1 < early and i - 1 < chips - 1:
            for q in range(1, PIECES):
                chain(i - 1, q)
    if chips > 1:
        paired(chips - 1)
    if chips < 3:
        sum_send(0)
        if halves > 1:
            shrink_rows(1)
    if halves > 1:
        sum_send(1)
    expand_rows(0)
    for turn in range(early, chips - 1):
        chain(turn, 0)
    if halves > 1:
        expand_rows(1)
    for turn in range(early, chips - 1):
        for q in range(1, PIECES):
            chain(turn, q)

    res_copy.wait()

    def branch_of(h, q, n):
        slot_col = slot_of(rank_col, own_col, h)
        unplace = jnp.where(
            lax.broadcasted_iota(jnp.int32, (rows, slots), 1) == slot_col, 1.0, 0.0
        ).astype(BF16)
        first = q * piece + n * tile
        back = eback[h, :, :, first:first + tile].reshape(slots, tile)
        return jnp.dot(unplace, back, preferred_element_type=F32)

    for h in range(halves):
        for k in range(1, groups):
            back_wait(h, k)
        for q in range(PIECES):
            for n in range(tiles):
                cols = slice(n * tile, (n + 1) * tile)
                first = q * piece + n * tile
                value = own[z * PIECES + q, :, cols] + branch_of(h, q, n)
                if h == 0:
                    value = (
                        value + precv[z * PIECES + q, :, cols].astype(F32)
                        + rbuf[:, first:first + tile].astype(F32)
                    )
                own[z * PIECES + q, :, cols] = value

    for q in range(PIECES):
        mine_at = z * PIECES + q

        def finish(use_right, use_left):
            @pl.loop(0, rows // strip)
            def _(n):
                at = pl.ds(pl.multiple_of(n * strip, strip), strip)
                value = own[mine_at, at]
                if use_right:
                    value = value + rrecv[mine_at, at].astype(F32)
                if use_left:
                    value = value + lrecv[mine_at, at].astype(F32)
                out_ref[at, q * piece:(q + 1) * piece] = value.astype(BF16)

        if chips == 1:
            finish(False, False)
        else:
            @pl.when(z == 0)
            def _():
                left(z, q, z).wait_recv()
                finish(False, True)

            @pl.when(z == chips - 1)
            def _():
                right(z, q, z).wait_recv()
                finish(True, False)

            @pl.when((z > 0) & (z < chips - 1))
            def _():
                right(z, q, z).wait_recv()
                left(z, q, z).wait_recv()
                finish(True, True)

    for i in range(chips):
        for q in range(PIECES):
            pair_copy(i, q).wait_send()
    for h in range(halves):
        for k in range(1, groups):
            row_copy(h, k).wait_send()
            back_copy(h, k).wait_send()
        term_pair(h).wait_send()
        for k in range(1, chips):
            term_copy(h, k).wait_send()
    for chip in range(chips):
        for q in range(PIECES):
            @pl.when(z < chip)
            def _():
                right(chip, q, z + 1).wait_send()

            @pl.when(z > chip)
            def _():
                left(chip, q, z - 1).wait_send()


def body(attention_output, residual, output_weight, down_factors, up_factors, adapter_index):
    groups = lax.axis_size("dp")
    members = lax.axis_size("tensor")
    rows, depth = attention_output.shape
    owned, _, rank = down_factors.shape
    width = output_weight.shape[1] // members
    cap = 2 * rows // groups
    chips = members // 2
    halves = 2 if cap % 32 == 0 else 1
    part = cap // halves
    slots = groups * part
    pack = slots * rank // LANES
    piece = width // PIECES
    down = jnp.swapaxes(down_factors, 1, 2).reshape(owned * rank, depth)
    up = up_factors.reshape(owned * rank, width)
    vmem = pl.BlockSpec(memory_space=pltpu.VMEM)
    hbm = pl.BlockSpec(memory_space=pl.ANY)
    dma = pltpu.SemaphoreType.DMA
    hops = chips * PIECES
    return pl.pallas_call(
        functools.partial(kernel, groups, members, rank, owned, halves),
        out_shape=jax.ShapeDtypeStruct((rows, width), BF16),
        in_specs=[vmem, hbm, vmem, hbm, hbm, hbm],
        out_specs=vmem,
        scratch_shapes=[
            pltpu.VMEM((members, depth, width), BF16),
            pltpu.VMEM((owned * rank, depth), BF16),
            pltpu.VMEM((owned * rank, width), BF16),
            pltpu.VMEM((rows, width), BF16),
            pltpu.VMEM((hops, rows, piece), F32),
            pltpu.VMEM((hops, rows, piece), BF16),
            pltpu.VMEM((hops, rows, piece), BF16),
            pltpu.VMEM((hops, rows, piece), BF16),
            pltpu.VMEM((hops, rows, piece), BF16),
            pltpu.VMEM((hops, rows, piece), BF16),
            pltpu.VMEM((hops, rows, piece), BF16),
            pltpu.VMEM((halves, groups, part, depth + LANES), BF16),
            pltpu.VMEM((halves, groups, part, depth + LANES), BF16),
            pltpu.VMEM((slots, LANES), F32),
            pltpu.VMEM((halves, pack, LANES), F32),
            pltpu.VMEM((halves, pack, LANES), F32),
            pltpu.VMEM((halves, chips, pack, LANES), F32),
            pltpu.VMEM((halves, groups, part, width), BF16),
            pltpu.VMEM((halves, groups, part, width), BF16),
            dma((members,)), dma((3,)),
            dma((hops,)), dma((hops,)),
            dma((hops,)), dma((hops,)), dma((hops,)), dma((hops,)),
            dma((halves * groups,)), dma((halves * groups,)),
            dma((halves,)), dma((halves,)),
            dma((halves * chips,)), dma((halves * chips,)),
            dma((halves * groups,)), dma((halves * groups,)),
        ],
        compiler_params=pltpu.CompilerParams(
            collective_id=0, has_side_effects=True, vmem_limit_bytes=60 * 1024 * 1024
        ),
    )(attention_output, residual, adapter_index.reshape(1, rows), output_weight, down, up)


def solution(mesh):
    return jax.shard_map(
        body,
        mesh=mesh,
        in_specs=(
            P("dp", "tensor"),
            P("dp", "tensor"),
            P("tensor", None),
            P("dp", "tensor", None),
            P("dp", None, "tensor"),
            P("dp"),
        ),
        out_specs=P("dp", "tensor"),
        check_vma=False,
    )
```
